32 devices in a mesh: rows: 32 (over z, y, x, core).
Axes of the slice: x: 2, y: 2, z: 4, core: 2. Of those that a mesh axis runs over, the one named last changes fastest.
Arguments:
- design: bfloat16 [131072, 1024], P('rows'), may hold values from -6 to 6
- weights: float32 [1024], replicated, may hold values from -0.1875 to 0.1875
- labels: int32 [131072], P('rows'), may hold values from 0 to 1
- signs: int32 [131072], P('rows'), may hold values from 0 to 1
- sample_rows: int32 [2048], replicated, may hold values from 0 to 131071
Outputs:
- gradient: float32 [1024], replicated
- newton_step: float32 [1024], replicated
- losses: float32 [4], replicated
The draws below stay inside these ranges and needn't reach their ends.
All inputs are finite; a program needn't handle non-finite values.
Results may differ from the reference program's by a relative error of at most 0.00085.
The reference program's roundings to bfloat16 on the way count: a program that leaves them out, or rounds other values in their place, can miss the bound.
Values may be sent and summed in bfloat16 or wider, within the bound.
A program may use at most 128 MiB of HBM per device.

```python
import jax
import jax.numpy as jnp
from jax import lax

WIDTH = 1024
ROWS_DEV = 4096
TOTAL_ROWS = 131072
SKETCH = 2048
N_ROWS = 32


def plant(drawn, rng, least, largest):
    longest = drawn.shape.index(max(drawn.shape))
    spots = []
    for shift in (0, 1):
        where = [jax.random.randint(jax.random.fold_in(rng, axis), (), 0, length) for axis, length in enumerate(drawn.shape)]
        where[longest] = (where[longest] + shift) % drawn.shape[longest]
        spots.append(tuple(where))
    return drawn.at[spots[0]].set(least).at[spots[1]].set(largest)


def shard_levels(rng, shape, split, low, largest):
    level, own = 1.0, jax.random.fold_in(rng, 6)
    for dim, parts in split:
        heights = jnp.exp(jax.random.uniform(jax.random.fold_in(own, dim), (parts,), jnp.float32, low / len(split), largest / len(split)))
        level = level * jnp.repeat(heights, shape[dim] // parts).reshape([-1 if axis == dim else 1 for axis in range(len(shape))])
    return level


def centred(key, shape, deviation, reach, cuts=(), kind=jnp.bfloat16):
    entries = deviation * jax.random.normal(key, shape, jnp.float32)
    if cuts:
        entries = entries * shard_levels(key, shape, cuts, -0.22, 0.18)
    return jnp.clip(entries, -reach, reach).astype(kind)


def setup_inputs(seed: int = 0) -> dict:
    keys = jax.random.split(jax.random.key(seed), 6)
    return {
        "design": centred(keys[0], (TOTAL_ROWS, WIDTH), 1.0, 6.0, ((0, 32),)),
        "weights": centred(keys[1], (WIDTH,), WIDTH ** -0.5, 0.1875, (), jnp.float32),
        "labels": plant(jax.random.randint(keys[2], (TOTAL_ROWS,), 0, 2), jax.random.fold_in(keys[2], 1), 0, 1).astype(jnp.int32),
        "signs": plant(jax.random.randint(keys[3], (TOTAL_ROWS,), 0, 2), jax.random.fold_in(keys[3], 1), 0, 1).astype(jnp.int32),
        "sample_rows": plant(jax.random.randint(keys[4], (SKETCH,), 0, TOTAL_ROWS), jax.random.fold_in(keys[4], 1), 0, TOTAL_ROWS - 1).astype(jnp.int32),
    }


ridge = 0.05

def hadamard(order_size):
    bits = order_size.bit_length() - 1
    row_index = lax.broadcasted_iota(jnp.int32, (order_size, order_size), 0)
    col_index = lax.broadcasted_iota(jnp.int32, (order_size, order_size), 1)
    parity = jnp.zeros((order_size, order_size), jnp.int32)
    for bit_number in range(bits):
        parity = parity + (row_index >> bit_number & 1) * (col_index >> bit_number & 1)
    return (1 - 2 * (parity % 2)).astype(jnp.float32)

def local_transform(scaled):
    rows_here, width = scaled.shape
    bits = rows_here.bit_length() - 1
    low_order = 1 << bits // 2
    high_order = rows_here // low_order
    high_matrix = hadamard(high_order).astype(jnp.bfloat16)
    first = jnp.dot(high_matrix.astype(jnp.float32), scaled.reshape(high_order, low_order * width).astype(jnp.float32), preferred_element_type=jnp.float32)
    low_matrix = hadamard(low_order)
    second = jnp.einsum('bx,axd->abd', low_matrix, first.reshape(high_order, low_order, width), precision=lax.Precision.HIGHEST)
    return second.reshape(rows_here, width)

def reference(design, weights, labels, signs, sample_rows):
    total_rows, width = design.shape
    margins = jnp.dot(design.astype(jnp.float32), weights.astype(jnp.bfloat16).astype(jnp.float32), preferred_element_type=jnp.float32)
    prob = jax.nn.sigmoid(margins)
    target = labels.astype(jnp.float32)
    misfit = (prob - target).astype(jnp.bfloat16)
    gradient = jnp.dot(misfit.astype(jnp.float32), design.astype(jnp.float32), preferred_element_type=jnp.float32) / total_rows + ridge * weights
    factor_rows = (1.0 - 2.0 * signs.astype(jnp.float32)) * jnp.sqrt(prob * (1.0 - prob))
    owner = sample_rows // ROWS_DEV
    local_rows = sample_rows % ROWS_DEV
    norm_factor = 1.0 / jnp.sqrt(jnp.float32(sample_rows.shape[0]))
    dev_bits = N_ROWS.bit_length() - 1

    def accumulate(carry, inputs):
        block, block_factor, device = inputs
        scaled = (block * block_factor[:, None]).astype(jnp.bfloat16)
        mixed = local_transform(scaled)
        parity = jnp.zeros(owner.shape, jnp.int32)
        for bit_number in range(dev_bits):
            parity = parity + (owner >> bit_number & 1) * (device >> bit_number & 1)
        coefs = (1 - 2 * (parity % 2)).astype(jnp.float32) * norm_factor
        return (carry + jnp.take(mixed, local_rows, axis=0) * coefs[:, None], None)
    blocks = design.reshape(N_ROWS, ROWS_DEV, width)
    factors = factor_rows.reshape(N_ROWS, ROWS_DEV)
    devices_list = jnp.arange(N_ROWS, dtype=jnp.int32)
    start_value = jnp.zeros((sample_rows.shape[0], width), jnp.float32)
    sketch_sum, unused = lax.scan(accumulate, start_value, (blocks, factors, devices_list))
    sketch = sketch_sum.astype(jnp.bfloat16)
    gram = jnp.dot(sketch.T.astype(jnp.float32), sketch.astype(jnp.float32), preferred_element_type=jnp.float32)
    hessian = gram / total_rows + ridge * jnp.eye(width, dtype=jnp.float32)
    cholesky_factor = jnp.linalg.cholesky(hessian)
    newton_step = jax.scipy.linalg.cho_solve((cholesky_factor, True), gradient)
    along = jnp.dot(design.astype(jnp.float32), newton_step.astype(jnp.bfloat16).astype(jnp.float32), preferred_element_type=jnp.float32)
    lengths = jnp.array([1.0, 0.5, 0.25, 0.125], jnp.float32)
    trial = margins[None, :] - lengths[:, None] * along[None, :]
    row_loss = jnp.logaddexp(0.0, trial) - target[None, :] * trial
    moved = weights[None, :] - lengths[:, None] * newton_step[None, :]
    losses = lax.optimization_barrier(jnp.sum(row_loss, axis=1)) / total_rows + 0.5 * ridge * lax.optimization_barrier(jnp.sum(moved * moved, axis=1))
    return (gradient, newton_step, losses)
```

```python
import functools

import jax
import jax.numpy as jnp
from jax import lax
from jax.experimental import pallas as pl
from jax.experimental.pallas import tpu as pltpu
from jax.sharding import PartitionSpec as P

ridge = 0.05
LANES = 128
MESH = pl.DeviceIdType.MESH


def parity_sign(bits):
    for shift in (16, 8, 4, 2, 1):
        bits = bits ^ (bits >> shift)
    return (1 - 2 * (bits & 1)).astype(jnp.float32)


def sampled_kernel(rows_here, picks_ref, scaled_ref, out_ref, matrix):
    me = lax.axis_index("rows")
    picks = picks_ref[...]
    tile = picks.shape[0]
    lane = lax.broadcasted_iota(jnp.int32, (tile, LANES), 1)
    chunks = rows_here // LANES
    local = picks & (rows_here - 1)
    owner_sign = parity_sign((picks >> (rows_here.bit_length() - 1)) & me)
    low = parity_sign(local & lane) * owner_sign
    high = parity_sign((local >> 7) & lane)
    for chunk in range(chunks):
        matrix[:, chunk * LANES : (chunk + 1) * LANES] = (
            low * high[:, chunk : chunk + 1]
        ).astype(jnp.bfloat16)
    out_ref[...] = jnp.dot(
        matrix[...], scaled_ref[...], preferred_element_type=jnp.float32
    )


def sampled_transform(picks, scaled):
    rows_here, width = scaled.shape
    total = picks.shape[0]
    tile = 256
    return pl.pallas_call(
        functools.partial(sampled_kernel, rows_here),
        grid=(total // tile,),
        out_shape=jax.ShapeDtypeStruct((total, width), jnp.float32),
        in_specs=[
            pl.BlockSpec((tile, 1), lambda i: (i, 0)),
            pl.BlockSpec((rows_here, width), lambda i: (0, 0)),
        ],
        out_specs=pl.BlockSpec((tile, width), lambda i: (i, 0)),
        scratch_shapes=[pltpu.VMEM((tile, rows_here), jnp.bfloat16)],
        name="sampled_transform",
    )(picks.reshape(total, 1), scaled)


def allsum_kernel(count, own_ref, out_ref, slots, send_sem, recv_sem):
    me = lax.axis_index("rows")
    barrier = pltpu.get_barrier_semaphore()

    @pl.loop(1, count)
    def greet(step):
        pl.semaphore_signal(
            barrier, inc=1, device_id=(lax.rem(me + step, count),), device_id_type=MESH
        )

    pl.semaphore_wait(barrier, count - 1)

    def copy(step):
        return pltpu.make_async_remote_copy(
            src_ref=own_ref,
            dst_ref=slots.at[me],
            send_sem=send_sem.at[step],
            recv_sem=recv_sem.at[step],
            device_id=(lax.rem(me + step, count),),
            device_id_type=MESH,
        )

    @pl.loop(1, count)
    def send(step):
        copy(step).start()

    slots[me] = own_ref[...]

    @pl.loop(1, count)
    def finish(step):
        copy(step).wait()

    out_ref[...] = jnp.sum(slots[...], axis=0)


def allsum(own, count, ident):
    return pl.pallas_call(
        functools.partial(allsum_kernel, count),
        out_shape=jax.ShapeDtypeStruct(own.shape, jnp.float32),
        in_specs=[pl.BlockSpec(memory_space=pltpu.VMEM)],
        out_specs=pl.BlockSpec(memory_space=pltpu.VMEM),
        scratch_shapes=[
            pltpu.VMEM((count,) + own.shape, jnp.float32),
            pltpu.SemaphoreType.DMA((count,)),
            pltpu.SemaphoreType.DMA((count,)),
        ],
        compiler_params=pltpu.CompilerParams(collective_id=ident, has_side_effects=True),
        name="allsum_%d" % ident,
    )(own)


def solve_kernel(total_rows, piece_ref, gradient_ref, step_ref, hess, vec_r, vec_p, vec_q):
    width = piece_ref.shape[1]
    block = 256
    scale = 1.0 / total_rows
    for start in range(0, width, block):
        gram = lax.dot_general(
            piece_ref[:, start : start + block],
            piece_ref[...],
            (((0,), (0,)), ((), ())),
            preferred_element_type=jnp.float32,
        )
        row = lax.broadcasted_iota(jnp.int32, (block, width), 0) + start
        col = lax.broadcasted_iota(jnp.int32, (block, width), 1)
        hess[start : start + block, :] = gram * scale + jnp.where(row == col, ridge, 0.0)
    diag = jnp.zeros((1, width), jnp.float32)
    for start in range(0, width, block):
        row = lax.broadcasted_iota(jnp.int32, (block, width), 0) + start
        col = lax.broadcasted_iota(jnp.int32, (block, width), 1)
        diag = diag + jnp.sum(
            jnp.where(row == col, hess[start : start + block, :], 0.0), axis=0, keepdims=True
        )
    inverse = 1.0 / diag
    right = gradient_ref[...]
    vec_r[...] = right
    start_z = right * inverse
    vec_p[...] = start_z
    step_ref[...] = jnp.zeros_like(right)
    start_rz = jnp.sum(right * start_z, axis=1, keepdims=True)
    goal = jnp.max(start_rz) * 1e-13

    def product():
        tiles = width // LANES
        sums = [jnp.zeros((8, LANES), jnp.float32) for tile in range(tiles)]
        for piece in range(tiles):
            span = slice(piece * LANES, (piece + 1) * LANES)
            column = jnp.broadcast_to(vec_p[:, span], (LANES, LANES)).T
            for tile in range(tiles):
                prod = hess[span, tile * LANES : (tile + 1) * LANES] * column
                sums[tile] = sums[tile] + jnp.sum(prod.reshape(LANES // 8, 8, LANES), axis=0)
        for tile in range(tiles):
            vec_q[:, tile * LANES : (tile + 1) * LANES] = jnp.sum(
                sums[tile], axis=0, keepdims=True
            )

    def go(carry):
        done, level, rz = carry
        return jnp.logical_and(level > goal, done < 8 * width)

    def advance(carry):
        done, level, rz = carry
        product()
        direction, image = vec_p[...], vec_q[...]
        curve = jnp.sum(direction * image, axis=1, keepdims=True)
        alpha = jnp.where(curve > 0.0, rz / curve, 0.0)
        step_ref[...] = step_ref[...] + alpha * direction
        rest = vec_r[...] - alpha * image
        vec_r[...] = rest
        scaled_rest = rest * inverse
        next_rz = jnp.sum(rest * scaled_rest, axis=1, keepdims=True)
        beta = jnp.where(rz > 0.0, next_rz / rz, 0.0)
        vec_p[...] = scaled_rest + beta * direction
        return done + 1, jnp.max(next_rz), next_rz

    lax.while_loop(go, advance, (jnp.int32(0), jnp.max(start_rz), start_rz))


def newton_solve(piece, gradient, total_rows):
    width = piece.shape[1]
    vector = pltpu.VMEM((1, width), jnp.float32)
    return pl.pallas_call(
        functools.partial(solve_kernel, total_rows),
        out_shape=jax.ShapeDtypeStruct((1, width), jnp.float32),
        in_specs=[pl.BlockSpec(memory_space=pltpu.VMEM)] * 2,
        out_specs=pl.BlockSpec(memory_space=pltpu.VMEM),
        scratch_shapes=[pltpu.VMEM((width, width), jnp.float32), vector, vector, vector],
        name="newton_solve",
    )(piece, gradient.reshape(1, width)).reshape(width)


def body(design, weights, labels, signs, sample_rows):
    rows_here, width = design.shape
    device_count = lax.axis_size("rows")
    total_rows = rows_here * device_count
    margins = jnp.dot(design, weights.astype(jnp.bfloat16), preferred_element_type=jnp.float32)
    prob = jax.nn.sigmoid(margins)
    target = labels.astype(jnp.float32)
    misfit = (prob - target).astype(jnp.bfloat16)
    grad_part = jnp.dot(misfit, design, preferred_element_type=jnp.float32)
    factor_rows = (1.0 - 2.0 * signs.astype(jnp.float32)) * jnp.sqrt(prob * (1.0 - prob))
    scaled = (design * factor_rows[:, None]).astype(jnp.bfloat16)
    grad_sum = allsum(grad_part.reshape(width // LANES, LANES), device_count, 0)
    gradient = grad_sum.reshape(width) / total_rows + ridge * weights
    norm_factor = 1.0 / jnp.sqrt(jnp.float32(sample_rows.shape[0]))
    own_part = sampled_transform(sample_rows, scaled)
    sketch_own = lax.psum_scatter(own_part, "rows", scatter_dimension=0, tiled=True)
    sketch_low = (sketch_own * norm_factor).astype(jnp.bfloat16)
    piece = lax.all_gather(sketch_low, "rows", axis=0, tiled=True)
    newton_step = newton_solve(piece, gradient, total_rows)
    along = jnp.dot(design, newton_step.astype(jnp.bfloat16), preferred_element_type=jnp.float32)
    lengths = jnp.array([1.0, 0.5, 0.25, 0.125], jnp.float32)
    trial = margins[None, :] - lengths[:, None] * along[None, :]
    row_loss = jnp.logaddexp(0.0, trial) - target[None, :] * trial
    loss_part = jnp.sum(row_loss, axis=1)
    loss_tile = jnp.broadcast_to(jnp.pad(loss_part, (0, 4))[:, None], (8, LANES))
    loss_total = allsum(loss_tile, device_count, 1)[:4, 0]
    moved = weights[None, :] - lengths[:, None] * newton_step[None, :]
    losses = loss_total / total_rows + 0.5 * ridge * jnp.sum(moved * moved, axis=1)
    return (gradient, newton_step, losses)


def solution(mesh):
    placed = (P("rows", None), P(), P("rows"), P("rows"), P())
    return jax.shard_map(
        body, mesh=mesh, in_specs=placed, out_specs=(P(), P(), P()), check_vma=False
    )
```

```python
import functools
import math

import jax
import jax.numpy as jnp
from jax import lax
from jax.experimental import pallas as pl
from jax.experimental.pallas import tpu as pltpu
from jax.sharding import PartitionSpec as P

ridge = 0.05
LANES = 128
MESH = pl.DeviceIdType.MESH


def parity_sign(bits):
    for shift in (16, 8, 4, 2, 1):
        bits = bits ^ (bits >> shift)
    return (1 - 2 * (bits & 1)).astype(jnp.float32)


def sampled_kernel(rows_here, picks_ref, scaled_ref, out_ref, matrix):
    me = lax.axis_index("rows")
    picks = picks_ref[...]
    tile = picks.shape[0]
    lane = lax.broadcasted_iota(jnp.int32, (tile, LANES), 1)
    chunks = rows_here // LANES
    local = picks & (rows_here - 1)
    owner_sign = parity_sign((picks >> (rows_here.bit_length() - 1)) & me)
    low = parity_sign(local & lane) * owner_sign
    high = parity_sign((local >> 7) & lane)
    for chunk in range(chunks):
        matrix[:, chunk * LANES : (chunk + 1) * LANES] = (
            low * high[:, chunk : chunk + 1]
        ).astype(jnp.bfloat16)
    out_ref[...] = jnp.dot(
        matrix[...], scaled_ref[...], preferred_element_type=jnp.float32
    )


def sampled_transform(picks, scaled):
    rows_here, width = scaled.shape
    total = picks.shape[0]
    tile = 256
    return pl.pallas_call(
        functools.partial(sampled_kernel, rows_here),
        grid=(total // tile,),
        out_shape=jax.ShapeDtypeStruct((total, width), jnp.float32),
        in_specs=[
            pl.BlockSpec((tile, 1), lambda i: (i, 0)),
            pl.BlockSpec((rows_here, width), lambda i: (0, 0)),
        ],
        out_specs=pl.BlockSpec((tile, width), lambda i: (i, 0)),
        scratch_shapes=[pltpu.VMEM((tile, rows_here), jnp.bfloat16)],
        name="sampled_transform",
    )(picks.reshape(total, 1), scaled)


def allsum_kernel(count, own_ref, out_ref, slots, send_sem, recv_sem):
    me = lax.axis_index("rows")
    barrier = pltpu.get_barrier_semaphore()

    @pl.loop(1, count)
    def greet(step):
        pl.semaphore_signal(
            barrier, inc=1, device_id=(lax.rem(me + step, count),), device_id_type=MESH
        )

    pl.semaphore_wait(barrier, count - 1)

    def copy(step):
        return pltpu.make_async_remote_copy(
            src_ref=own_ref,
            dst_ref=slots.at[me],
            send_sem=send_sem.at[step],
            recv_sem=recv_sem.at[step],
            device_id=(lax.rem(me + step, count),),
            device_id_type=MESH,
        )

    @pl.loop(1, count)
    def send(step):
        copy(step).start()

    slots[me] = own_ref[...]

    @pl.loop(1, count)
    def finish(step):
        copy(step).wait()

    out_ref[...] = jnp.sum(slots[...], axis=0)


def allsum(own, count, ident):
    return pl.pallas_call(
        functools.partial(allsum_kernel, count),
        out_shape=jax.ShapeDtypeStruct(own.shape, jnp.float32),
        in_specs=[pl.BlockSpec(memory_space=pltpu.VMEM)],
        out_specs=pl.BlockSpec(memory_space=pltpu.VMEM),
        scratch_shapes=[
            pltpu.VMEM((count,) + own.shape, jnp.float32),
            pltpu.SemaphoreType.DMA((count,)),
            pltpu.SemaphoreType.DMA((count,)),
        ],
        compiler_params=pltpu.CompilerParams(collective_id=ident, has_side_effects=True),
        name="allsum_%d" % ident,
    )(own)


def exchange_kernel(
    orders, spans, part_ref, grad_ref, sketch_ref, gsum_ref,
    total, arrive_first, arrive_rest, grad_slots, grad_own,
    send_sem, recv_sem, back_send, back_recv, grad_send, grad_recv,
):
    me = lax.axis_index("rows")
    steps = len(orders[0])
    rows = part_ref.shape[0]
    norm = 1.0 / math.sqrt(rows)
    half = rows // 2
    groups = range(len(orders))

    def peer(bit):
        return me ^ (1 << bit)

    def mine(bit):
        return (me >> bit) & 1

    barrier = pltpu.get_barrier_semaphore()
    for bit in range(steps):
        pl.semaphore_signal(barrier, inc=1, device_id=(peer(bit),), device_id_type=MESH)
    pl.semaphore_wait(barrier, steps)

    def remote(source, target, out_sem, in_sem, bit):
        return pltpu.make_async_remote_copy(
            src_ref=source, dst_ref=target, send_sem=out_sem, recv_sem=in_sem,
            device_id=(peer(bit),), device_id_type=MESH,
        )

    core = orders[0][0]
    base = pl.multiple_of(mine(core) * half, half)
    other = pl.multiple_of((1 - mine(core)) * half, half)
    sent = []
    pending = {}

    def start(copy, key):
        copy.start()
        sent.append(copy)
        pending[key] = copy

    def grad_start(step):
        source = grad_ref if step == 0 else grad_own.at[step - 1]
        start(
            remote(source, grad_slots.at[step], grad_send.at[step], grad_recv.at[step], step),
            ("grad", step),
        )

    def grad_finish(step):
        pending[("grad", step)].wait_recv()
        before = grad_ref[...] if step == 0 else grad_own[step - 1]
        grad_own[step] = before + grad_slots[step]

    grad_start(0)
    for group in groups:
        cols = slice(*spans[group])
        start(
            remote(
                part_ref.at[pl.ds(other, half), cols], arrive_first.at[:, cols],
                send_sem.at[0, group], recv_sem.at[0, group], core,
            ),
            (0, group),
        )

    offsets = [0 for group in groups]
    history = [[] for group in groups]

    def rest_start(step, group):
        cols = slice(*spans[group])
        size = half >> step
        bit = orders[group][step]
        place = half - (half >> (step - 1))
        history[group].append(offsets[group])
        away = pl.multiple_of(offsets[group] + (1 - mine(bit)) * size, size)
        start(
            remote(
                total.at[pl.ds(away, size), cols], arrive_rest.at[pl.ds(place, size), cols],
                send_sem.at[step, group], recv_sem.at[step, group], bit,
            ),
            (step, group),
        )
        offsets[group] = pl.multiple_of(offsets[group] + mine(bit) * size, size)

    for step in range(steps):
        if step > 0:
            grad_start(step)
        for group in groups:
            cols = slice(*spans[group])
            pending[(step, group)].wait_recv()
            if step == 0:
                total[:, cols] = part_ref[pl.ds(base, half), cols] + arrive_first[:, cols]
            else:
                size = half >> step
                place = half - (half >> (step - 1))
                keep = pl.ds(offsets[group], size)
                total[keep, cols] = total[keep, cols] + arrive_rest[place : place + size, cols]
            if step + 1 < steps:
                rest_start(step + 1, group)
        grad_finish(step)

    def back_start(step, group):
        cols = slice(*spans[group])
        bit = orders[group][step]
        size = half >> step
        place = pl.ds(pl.multiple_of(base + offsets[group], size), size)
        start(
            remote(
                sketch_ref.at[place, cols], sketch_ref.at[place, cols],
                back_send.at[step, group], back_recv.at[step, group], bit,
            ),
            ("back", step, group),
        )

    last = half >> (steps - 1)
    for group in groups:
        cols = slice(*spans[group])
        place = pl.ds(pl.multiple_of(base + offsets[group], last), last)
        sketch_ref[place, cols] = (total[pl.ds(offsets[group], last), cols] * norm).astype(
            sketch_ref.dtype
        )
        back_start(steps - 1, group)
    for step in range(steps - 1, -1, -1):
        for group in groups:
            pending[("back", step, group)].wait_recv()
            if step > 0:
                offsets[group] = history[group][step - 1]
                back_start(step - 1, group)
    gsum_ref[...] = grad_own[steps - 1]
    for copy in sent:
        copy.wait_send()


def exchange(part, grad, count):
    rows, width = part.shape
    bits = count.bit_length() - 1
    rest = list(range(1, bits))
    tiles = width // LANES
    lanes = 3
    cuts = [-(-tiles * group // lanes) * LANES for group in range(lanes + 1)]
    spans = [(cuts[group], cuts[group + 1]) for group in range(lanes)]
    orders = []
    for group in range(lanes):
        turn = group * len(rest) // lanes
        orders.append([0] + rest[turn:] + rest[:turn])
    grid_sem = pltpu.SemaphoreType.DMA((bits, lanes))
    line_sem = pltpu.SemaphoreType.DMA((bits,))
    vmem = pl.BlockSpec(memory_space=pltpu.VMEM)
    return pl.pallas_call(
        functools.partial(exchange_kernel, orders, spans),
        out_shape=(
            jax.ShapeDtypeStruct((rows, width), jnp.bfloat16),
            jax.ShapeDtypeStruct(grad.shape, jnp.float32),
        ),
        in_specs=[vmem, vmem],
        out_specs=(vmem, vmem),
        scratch_shapes=[
            pltpu.VMEM((rows // 2, width), jnp.float32),
            pltpu.VMEM((rows // 2, width), jnp.float32),
            pltpu.VMEM((rows // 2, width), jnp.float32),
            pltpu.VMEM((bits,) + grad.shape, jnp.float32),
            pltpu.VMEM((bits,) + grad.shape, jnp.float32),
            grid_sem, grid_sem, grid_sem, grid_sem, line_sem, line_sem,
        ],
        compiler_params=pltpu.CompilerParams(collective_id=2, has_side_effects=True),
        name="exchange",
    )(part, grad)


def solve_kernel(total_rows, piece_ref, gradient_ref, step_ref, hess, vec_r, vec_p, vec_q):
    width = piece_ref.shape[1]
    block = 256
    scale = 1.0 / total_rows
    for start in range(0, width, block):
        gram = lax.dot_general(
            piece_ref[:, start : start + block],
            piece_ref[...],
            (((0,), (0,)), ((), ())),
            preferred_element_type=jnp.float32,
        )
        row = lax.broadcasted_iota(jnp.int32, (block, width), 0) + start
        col = lax.broadcasted_iota(jnp.int32, (block, width), 1)
        hess[start : start + block, :] = gram * scale + jnp.where(row == col, ridge, 0.0)
    diag = jnp.zeros((1, width), jnp.float32)
    for start in range(0, width, block):
        row = lax.broadcasted_iota(jnp.int32, (block, width), 0) + start
        col = lax.broadcasted_iota(jnp.int32, (block, width), 1)
        diag = diag + jnp.sum(
            jnp.where(row == col, hess[start : start + block, :], 0.0), axis=0, keepdims=True
        )
    inverse = 1.0 / diag
    right = gradient_ref[...]
    vec_r[...] = right
    start_z = right * inverse
    vec_p[...] = start_z
    step_ref[...] = jnp.zeros_like(right)
    start_rz = jnp.sum(right * start_z, axis=1, keepdims=True)
    goal = jnp.max(start_rz) * 1e-13

    def product():
        tiles = width // LANES
        sums = [jnp.zeros((8, LANES), jnp.float32) for tile in range(tiles)]
        for piece in range(tiles):
            span = slice(piece * LANES, (piece + 1) * LANES)
            column = jnp.broadcast_to(vec_p[:, span], (LANES, LANES)).T
            for tile in range(tiles):
                prod = hess[span, tile * LANES : (tile + 1) * LANES] * column
                sums[tile] = sums[tile] + jnp.sum(prod.reshape(LANES // 8, 8, LANES), axis=0)
        for tile in range(tiles):
            vec_q[:, tile * LANES : (tile + 1) * LANES] = jnp.sum(
                sums[tile], axis=0, keepdims=True
            )

    def go(carry):
        done, level, rz = carry
        return jnp.logical_and(level > goal, done < 8 * width)

    def advance(carry):
        done, level, rz = carry
        product()
        direction, image = vec_p[...], vec_q[...]
        curve = jnp.sum(direction * image, axis=1, keepdims=True)
        alpha = jnp.where(curve > 0.0, rz / curve, 0.0)
        step_ref[...] = step_ref[...] + alpha * direction
        rest = vec_r[...] - alpha * image
        vec_r[...] = rest
        scaled_rest = rest * inverse
        next_rz = jnp.sum(rest * scaled_rest, axis=1, keepdims=True)
        beta = jnp.where(rz > 0.0, next_rz / rz, 0.0)
        vec_p[...] = scaled_rest + beta * direction
        return done + 1, jnp.max(next_rz), next_rz

    lax.while_loop(go, advance, (jnp.int32(0), jnp.max(start_rz), start_rz))


def newton_solve(piece, gradient, total_rows):
    width = piece.shape[1]
    vector = pltpu.VMEM((1, width), jnp.float32)
    return pl.pallas_call(
        functools.partial(solve_kernel, total_rows),
        out_shape=jax.ShapeDtypeStruct((1, width), jnp.float32),
        in_specs=[pl.BlockSpec(memory_space=pltpu.VMEM)] * 2,
        out_specs=pl.BlockSpec(memory_space=pltpu.VMEM),
        scratch_shapes=[pltpu.VMEM((width, width), jnp.float32), vector, vector, vector],
        name="newton_solve",
    )(piece, gradient.reshape(1, width)).reshape(width)


def body(design, weights, labels, signs, sample_rows):
    rows_here, width = design.shape
    device_count = lax.axis_size("rows")
    total_rows = rows_here * device_count
    margins = jnp.dot(design, weights.astype(jnp.bfloat16), preferred_element_type=jnp.float32)
    prob = jax.nn.sigmoid(margins)
    target = labels.astype(jnp.float32)
    misfit = (prob - target).astype(jnp.bfloat16)
    grad_part = jnp.dot(misfit, design, preferred_element_type=jnp.float32)
    factor_rows = (1.0 - 2.0 * signs.astype(jnp.float32)) * jnp.sqrt(prob * (1.0 - prob))
    scaled = (design * factor_rows[:, None]).astype(jnp.bfloat16)
    own_part = sampled_transform(sample_rows, scaled)
    piece, grad_sum = exchange(
        own_part, grad_part.reshape(width // LANES, LANES), device_count
    )
    gradient = grad_sum.reshape(width) / total_rows + ridge * weights
    newton_step = newton_solve(piece, gradient, total_rows)
    along = jnp.dot(design, newton_step.astype(jnp.bfloat16), preferred_element_type=jnp.float32)
    lengths = jnp.array([1.0, 0.5, 0.25, 0.125], jnp.float32)
    trial = margins[None, :] - lengths[:, None] * along[None, :]
    row_loss = jnp.logaddexp(0.0, trial) - target[None, :] * trial
    loss_part = jnp.sum(row_loss, axis=1)
    loss_tile = jnp.broadcast_to(jnp.pad(loss_part, (0, 4))[:, None], (8, LANES))
    loss_total = allsum(loss_tile, device_count, 1)[:4, 0]
    moved = weights[None, :] - lengths[:, None] * newton_step[None, :]
    losses = loss_total / total_rows + 0.5 * ridge * jnp.sum(moved * moved, axis=1)
    return (gradient, newton_step, losses)


def solution(mesh):
    placed = (P("rows", None), P(), P("rows"), P("rows"), P())
    return jax.shard_map(
        body, mesh=mesh, in_specs=placed, out_specs=(P(), P(), P()), check_vma=False
    )
```

```python
import functools
import math

import jax
import jax.numpy as jnp
from jax import lax
from jax.experimental import pallas as pl
from jax.experimental.pallas import tpu as pltpu
from jax.sharding import PartitionSpec as P

ridge = 0.05
LANES = 128
MESH = pl.DeviceIdType.MESH


def parity_sign(bits):
    for shift in (16, 8, 4, 2, 1):
        bits = bits ^ (bits >> shift)
    return (1 - 2 * (bits & 1)).astype(jnp.float32)


def front_kernel(
    steps, picks_ref, picks_sign_ref, design_ref, weights_ref, labels_ref, signs_ref,
    margins_ref, grad_ref, out_ref, matrix, mixed,
):
    step = pl.program_id(0)
    block, width = design_ref.shape
    tiles = width // LANES

    @pl.when(step == 0)
    def prepare():
        row = lax.broadcasted_iota(jnp.int32, (block, block), 0)
        col = lax.broadcasted_iota(jnp.int32, (block, block), 1)
        matrix[...] = parity_sign(row & col).astype(jnp.bfloat16)
        grad_ref[...] = jnp.zeros_like(grad_ref)

    weights = jnp.broadcast_to(weights_ref[...], (LANES, width)).astype(jnp.bfloat16)
    spread = lax.dot_general(
        design_ref[...], weights, (((1,), (1,)), ((), ())), preferred_element_type=jnp.float32
    )
    parts = []
    for piece in range(block // LANES):
        span = slice(piece * LANES, (piece + 1) * LANES)
        margin = spread[span, :].T[:8, :]
        margins_ref[0, piece : piece + 1, :] = margin[:1, :]
        prob = 1.0 / (1.0 + jnp.exp(-margin))
        label = labels_ref[0, piece : piece + 1, :].astype(jnp.float32)
        sign = signs_ref[0, piece : piece + 1, :].astype(jnp.float32)
        misfit = (prob - label).astype(jnp.bfloat16)
        grad_ref[...] += jnp.dot(
            misfit, design_ref[span, :], preferred_element_type=jnp.float32
        )
        factor = ((1.0 - 2.0 * sign) * jnp.sqrt(prob * (1.0 - prob)))[:1, :]
        column = jnp.broadcast_to(factor, (LANES, LANES)).T
        wide = jnp.concatenate([column] * tiles, axis=1)
        parts.append((design_ref[span, :].astype(jnp.float32) * wide).astype(jnp.bfloat16))
    scaled = jnp.concatenate(parts, axis=0)
    mixed[pl.ds(pl.multiple_of(step * block, block), block), :] = jnp.dot(
        matrix[...], scaled, preferred_element_type=jnp.float32
    )

    @pl.when(step == steps - 1)
    def finish():
        @pl.loop(0, block // 8)
        def butterfly(group):
            for tile in range(tiles):
                cols = slice(tile * LANES, (tile + 1) * LANES)
                spots = [
                    pl.ds(pl.multiple_of(index * block + group * 8, 8), 8)
                    for index in range(steps)
                ]
                values = [mixed[spot, cols] for spot in spots]
                gap = 1
                while gap < steps:
                    for index in range(steps):
                        if not index & gap:
                            above, below = values[index], values[index + gap]
                            values[index] = above + below
                            values[index + gap] = above - below
                    gap *= 2
                for spot, value in zip(spots, values):
                    mixed[spot, cols] = value

        @pl.loop(0, out_ref.shape[0] // 8)
        def gather(group):
            for lane in range(8):
                place = group * 8 + lane
                row = mixed[pl.ds(picks_ref[place], 1), :]
                out_ref[pl.ds(place, 1), :] = row * picks_sign_ref[place]


def front(design, weights, labels, signs, picks, picks_sign):
    rows_here, width = design.shape
    total = picks.shape[0]
    block = 256
    steps = rows_here // block
    lines = (steps, block // LANES, LANES)
    smem = pl.BlockSpec(memory_space=pltpu.SMEM)
    line = pl.BlockSpec((1,) + lines[1:], lambda i: (i, 0, 0))
    return pl.pallas_call(
        functools.partial(front_kernel, steps),
        grid=(steps,),
        out_shape=(
            jax.ShapeDtypeStruct(lines, jnp.float32),
            jax.ShapeDtypeStruct((8, width), jnp.float32),
            jax.ShapeDtypeStruct((total, width), jnp.float32),
        ),
        in_specs=[
            smem,
            smem,
            pl.BlockSpec((block, width), lambda i: (i, 0)),
            pl.BlockSpec((1, width), lambda i: (0, 0)),
            line,
            line,
        ],
        out_specs=(
            line,
            pl.BlockSpec((8, width), lambda i: (0, 0)),
            pl.BlockSpec((total, width), lambda i: (0, 0)),
        ),
        scratch_shapes=[
            pltpu.VMEM((block, block), jnp.bfloat16),
            pltpu.VMEM((rows_here, width), jnp.float32),
        ],
        name="front",
    )(picks, picks_sign, design, weights.reshape(1, width), labels.reshape(lines), signs.reshape(lines))


def allsum_kernel(count, own_ref, out_ref, slots, send_sem, recv_sem):
    me = lax.axis_index("rows")
    barrier = pltpu.get_barrier_semaphore()

    @pl.loop(1, count)
    def greet(step):
        pl.semaphore_signal(
            barrier, inc=1, device_id=(lax.rem(me + step, count),), device_id_type=MESH
        )

    pl.semaphore_wait(barrier, count - 1)

    def copy(step):
        return pltpu.make_async_remote_copy(
            src_ref=own_ref,
            dst_ref=slots.at[me],
            send_sem=send_sem.at[step],
            recv_sem=recv_sem.at[step],
            device_id=(lax.rem(me + step, count),),
            device_id_type=MESH,
        )

    @pl.loop(1, count)
    def send(step):
        copy(step).start()

    slots[me] = own_ref[...]

    @pl.loop(1, count)
    def finish(step):
        copy(step).wait()

    out_ref[...] = jnp.sum(slots[...], axis=0)


def allsum(own, count, ident):
    return pl.pallas_call(
        functools.partial(allsum_kernel, count),
        out_shape=jax.ShapeDtypeStruct(own.shape, jnp.float32),
        in_specs=[pl.BlockSpec(memory_space=pltpu.VMEM)],
        out_specs=pl.BlockSpec(memory_space=pltpu.VMEM),
        scratch_shapes=[
            pltpu.VMEM((count,) + own.shape, jnp.float32),
            pltpu.SemaphoreType.DMA((count,)),
            pltpu.SemaphoreType.DMA((count,)),
        ],
        compiler_params=pltpu.CompilerParams(collective_id=ident, has_side_effects=True),
        name="allsum_%d" % ident,
    )(own)


def exchange_kernel(
    orders, spans, part_ref, grad_ref, sketch_ref, gsum_ref,
    total, arrive_first, arrive_rest, grad_slots, grad_own,
    send_sem, recv_sem, back_send, back_recv, grad_send, grad_recv,
):
    me = lax.axis_index("rows")
    steps = len(orders[0])
    rows = part_ref.shape[0]
    norm = 1.0 / math.sqrt(rows)
    half = rows // 2
    groups = range(len(orders))

    def peer(bit):
        return me ^ (1 << bit)

    def mine(bit):
        return (me >> bit) & 1

    barrier = pltpu.get_barrier_semaphore()
    for bit in range(steps):
        pl.semaphore_signal(barrier, inc=1, device_id=(peer(bit),), device_id_type=MESH)
    pl.semaphore_wait(barrier, steps)

    def remote(source, target, out_sem, in_sem, bit):
        return pltpu.make_async_remote_copy(
            src_ref=source, dst_ref=target, send_sem=out_sem, recv_sem=in_sem,
            device_id=(peer(bit),), device_id_type=MESH,
        )

    core = orders[0][0]
    base = pl.multiple_of(mine(core) * half, half)
    other = pl.multiple_of((1 - mine(core)) * half, half)
    sent = []
    pending = {}

    def start(copy, key):
        copy.start()
        sent.append(copy)
        pending[key] = copy

    def grad_start(step):
        source = grad_ref if step == 0 else grad_own.at[step - 1]
        start(
            remote(source, grad_slots.at[step], grad_send.at[step], grad_recv.at[step], step),
            ("grad", step),
        )

    def grad_finish(step):
        pending[("grad", step)].wait_recv()
        before = grad_ref[...] if step == 0 else grad_own[step - 1]
        grad_own[step] = before + grad_slots[step]

    grad_start(0)
    for group in groups:
        cols = slice(*spans[group])
        start(
            remote(
                part_ref.at[pl.ds(other, half), cols], arrive_first.at[:, cols],
                send_sem.at[0, group], recv_sem.at[0, group], core,
            ),
            (0, group),
        )

    offsets = [0 for group in groups]
    history = [[] for group in groups]

    def rest_start(step, group):
        cols = slice(*spans[group])
        size = half >> step
        bit = orders[group][step]
        place = half - (half >> (step - 1))
        history[group].append(offsets[group])
        away = pl.multiple_of(offsets[group] + (1 - mine(bit)) * size, size)
        start(
            remote(
                total.at[pl.ds(away, size), cols], arrive_rest.at[pl.ds(place, size), cols],
                send_sem.at[step, group], recv_sem.at[step, group], bit,
            ),
            (step, group),
        )
        offsets[group] = pl.multiple_of(offsets[group] + mine(bit) * size, size)

    for step in range(steps):
        if step > 0:
            grad_start(step)
        for group in groups:
            cols = slice(*spans[group])
            pending[(step, group)].wait_recv()
            if step == 0:
                total[:, cols] = part_ref[pl.ds(base, half), cols] + arrive_first[:, cols]
            else:
                size = half >> step
                place = half - (half >> (step - 1))
                keep = pl.ds(offsets[group], size)
                total[keep, cols] = total[keep, cols] + arrive_rest[place : place + size, cols]
            if step + 1 < steps:
                rest_start(step + 1, group)
        grad_finish(step)

    def back_start(step, group):
        cols = slice(*spans[group])
        bit = orders[group][step]
        size = half >> step
        place = pl.ds(pl.multiple_of(base + offsets[group], size), size)
        start(
            remote(
                sketch_ref.at[place, cols], sketch_ref.at[place, cols],
                back_send.at[step, group], back_recv.at[step, group], bit,
            ),
            ("back", step, group),
        )

    last = half >> (steps - 1)
    for group in groups:
        cols = slice(*spans[group])
        place = pl.ds(pl.multiple_of(base + offsets[group], last), last)
        sketch_ref[place, cols] = (total[pl.ds(offsets[group], last), cols] * norm).astype(
            sketch_ref.dtype
        )
        back_start(steps - 1, group)
    for step in range(steps - 1, -1, -1):
        for group in groups:
            pending[("back", step, group)].wait_recv()
            if step > 0:
                offsets[group] = history[group][step - 1]
                back_start(step - 1, group)
    gsum_ref[...] = grad_own[steps - 1]
    for copy in sent:
        copy.wait_send()


def exchange(part, grad, count):
    rows, width = part.shape
    bits = count.bit_length() - 1
    rest = list(range(1, bits))
    tiles = width // LANES
    lanes = 3
    cuts = [-(-tiles * group // lanes) * LANES for group in range(lanes + 1)]
    spans = [(cuts[group], cuts[group + 1]) for group in range(lanes)]
    orders = []
    for group in range(lanes):
        turn = group * len(rest) // lanes
        orders.append([0] + rest[turn:] + rest[:turn])
    grid_sem = pltpu.SemaphoreType.DMA((bits, lanes))
    line_sem = pltpu.SemaphoreType.DMA((bits,))
    vmem = pl.BlockSpec(memory_space=pltpu.VMEM)
    return pl.pallas_call(
        functools.partial(exchange_kernel, orders, spans),
        out_shape=(
            jax.ShapeDtypeStruct((rows, width), jnp.bfloat16),
            jax.ShapeDtypeStruct(grad.shape, jnp.float32),
        ),
        in_specs=[vmem, vmem],
        out_specs=(vmem, vmem),
        scratch_shapes=[
            pltpu.VMEM((rows // 2, width), jnp.float32),
            pltpu.VMEM((rows // 2, width), jnp.float32),
            pltpu.VMEM((rows // 2, width), jnp.float32),
            pltpu.VMEM((bits,) + grad.shape, jnp.float32),
            pltpu.VMEM((bits,) + grad.shape, jnp.float32),
            grid_sem, grid_sem, grid_sem, grid_sem, line_sem, line_sem,
        ],
        compiler_params=pltpu.CompilerParams(collective_id=2, has_side_effects=True),
        name="exchange",
    )(part, grad)


def solve_kernel(total_rows, piece_ref, gradient_ref, step_ref, hess, vec_r, vec_p, vec_q):
    width = piece_ref.shape[1]
    block = 256
    scale = 1.0 / total_rows
    for start in range(0, width, block):
        gram = lax.dot_general(
            piece_ref[:, start : start + block],
            piece_ref[...],
            (((0,), (0,)), ((), ())),
            preferred_element_type=jnp.float32,
        )
        row = lax.broadcasted_iota(jnp.int32, (block, width), 0) + start
        col = lax.broadcasted_iota(jnp.int32, (block, width), 1)
        hess[start : start + block, :] = gram * scale + jnp.where(row == col, ridge, 0.0)
    diag = jnp.zeros((1, width), jnp.float32)
    for start in range(0, width, block):
        row = lax.broadcasted_iota(jnp.int32, (block, width), 0) + start
        col = lax.broadcasted_iota(jnp.int32, (block, width), 1)
        diag = diag + jnp.sum(
            jnp.where(row == col, hess[start : start + block, :], 0.0), axis=0, keepdims=True
        )
    inverse = 1.0 / diag
    right = gradient_ref[...]
    vec_r[...] = right
    start_z = right * inverse
    vec_p[...] = start_z
    step_ref[...] = jnp.zeros_like(right)
    start_rz = jnp.sum(right * start_z, axis=1, keepdims=True)
    goal = jnp.max(start_rz) * 1e-13

    def product():
        tiles = width // LANES
        sums = [jnp.zeros((8, LANES), jnp.float32) for tile in range(tiles)]
        for piece in range(tiles):
            span = slice(piece * LANES, (piece + 1) * LANES)
            column = jnp.broadcast_to(vec_p[:, span], (LANES, LANES)).T
            for tile in range(tiles):
                prod = hess[span, tile * LANES : (tile + 1) * LANES] * column
                sums[tile] = sums[tile] + jnp.sum(prod.reshape(LANES // 8, 8, LANES), axis=0)
        for tile in range(tiles):
            vec_q[:, tile * LANES : (tile + 1) * LANES] = jnp.sum(
                sums[tile], axis=0, keepdims=True
            )

    def go(carry):
        done, level, rz = carry
        return jnp.logical_and(level > goal, done < 8 * width)

    def advance(carry):
        done, level, rz = carry
        product()
        direction, image = vec_p[...], vec_q[...]
        curve = jnp.sum(direction * image, axis=1, keepdims=True)
        alpha = jnp.where(curve > 0.0, rz / curve, 0.0)
        step_ref[...] = step_ref[...] + alpha * direction
        rest = vec_r[...] - alpha * image
        vec_r[...] = rest
        scaled_rest = rest * inverse
        next_rz = jnp.sum(rest * scaled_rest, axis=1, keepdims=True)
        beta = jnp.where(rz > 0.0, next_rz / rz, 0.0)
        vec_p[...] = scaled_rest + beta * direction
        return done + 1, jnp.max(next_rz), next_rz

    lax.while_loop(go, advance, (jnp.int32(0), jnp.max(start_rz), start_rz))


def newton_solve(piece, gradient, total_rows):
    width = piece.shape[1]
    vector = pltpu.VMEM((1, width), jnp.float32)
    return pl.pallas_call(
        functools.partial(solve_kernel, total_rows),
        out_shape=jax.ShapeDtypeStruct((1, width), jnp.float32),
        in_specs=[pl.BlockSpec(memory_space=pltpu.VMEM)] * 2,
        out_specs=pl.BlockSpec(memory_space=pltpu.VMEM),
        scratch_shapes=[pltpu.VMEM((width, width), jnp.float32), vector, vector, vector],
        name="newton_solve",
    )(piece, gradient.reshape(1, width)).reshape(width)


def body(design, weights, labels, signs, sample_rows):
    rows_here, width = design.shape
    device_count = lax.axis_size("rows")
    total_rows = rows_here * device_count
    owner_sign = parity_sign((sample_rows // rows_here) & lax.axis_index("rows"))
    margins, grad_part, own_part = front(
        design, weights, labels, signs, sample_rows % rows_here, owner_sign
    )
    margins = margins.reshape(rows_here)
    target = labels.astype(jnp.float32)
    piece, grad_sum = exchange(
        own_part, grad_part[0].reshape(width // LANES, LANES), device_count
    )
    gradient = grad_sum.reshape(width) / total_rows + ridge * weights
    newton_step = newton_solve(piece, gradient, total_rows)
    along = jnp.dot(design, newton_step.astype(jnp.bfloat16), preferred_element_type=jnp.float32)
    lengths = jnp.array([1.0, 0.5, 0.25, 0.125], jnp.float32)
    trial = margins[None, :] - lengths[:, None] * along[None, :]
    row_loss = jnp.logaddexp(0.0, trial) - target[None, :] * trial
    loss_part = jnp.sum(row_loss, axis=1)
    loss_tile = jnp.broadcast_to(jnp.pad(loss_part, (0, 4))[:, None], (8, LANES))
    loss_total = allsum(loss_tile, device_count, 1)[:4, 0]
    moved = weights[None, :] - lengths[:, None] * newton_step[None, :]
    losses = loss_total / total_rows + 0.5 * ridge * jnp.sum(moved * moved, axis=1)
    return (gradient, newton_step, losses)


def solution(mesh):
    placed = (P("rows", None), P(), P("rows"), P("rows"), P())
    return jax.shard_map(
        body, mesh=mesh, in_specs=placed, out_specs=(P(), P(), P()), check_vma=False
    )
```

```python
import functools
import math

import jax
import jax.numpy as jnp
from jax import lax
from jax.experimental import pallas as pl
from jax.experimental.pallas import tpu as pltpu
from jax.sharding import PartitionSpec as P

ridge = 0.05
LANES = 128
MESH = pl.DeviceIdType.MESH


def parity_sign(bits):
    for shift in (16, 8, 4, 2, 1):
        bits = bits ^ (bits >> shift)
    return (1 - 2 * (bits & 1)).astype(jnp.float32)


def front_kernel(
    steps, picks_ref, picks_sign_ref, design_ref, weights_ref, labels_ref, signs_ref,
    margins_ref, grad_ref, out_ref, matrix, mixed,
):
    step = pl.program_id(0)
    block, width = design_ref.shape
    tiles = width // LANES

    @pl.when(step == 0)
    def prepare():
        row = lax.broadcasted_iota(jnp.int32, (block, block), 0)
        col = lax.broadcasted_iota(jnp.int32, (block, block), 1)
        matrix[...] = parity_sign(row & col).astype(jnp.bfloat16)
        grad_ref[...] = jnp.zeros_like(grad_ref)

    weights = jnp.broadcast_to(weights_ref[...], (LANES, width)).astype(jnp.bfloat16)
    spread = lax.dot_general(
        design_ref[...], weights, (((1,), (1,)), ((), ())), preferred_element_type=jnp.float32
    )
    parts = []
    for piece in range(block // LANES):
        span = slice(piece * LANES, (piece + 1) * LANES)
        margin = spread[span, :].T[:8, :]
        margins_ref[0, piece : piece + 1, :] = margin[:1, :]
        prob = 1.0 / (1.0 + jnp.exp(-margin))
        label = labels_ref[0, piece : piece + 1, :].astype(jnp.float32)
        sign = signs_ref[0, piece : piece + 1, :].astype(jnp.float32)
        misfit = (prob - label).astype(jnp.bfloat16)
        grad_ref[...] += jnp.dot(
            misfit, design_ref[span, :], preferred_element_type=jnp.float32
        )
        factor = ((1.0 - 2.0 * sign) * jnp.sqrt(prob * (1.0 - prob)))[:1, :]
        column = jnp.broadcast_to(factor, (LANES, LANES)).T
        wide = jnp.concatenate([column] * tiles, axis=1)
        parts.append((design_ref[span, :].astype(jnp.float32) * wide).astype(jnp.bfloat16))
    scaled = jnp.concatenate(parts, axis=0)
    mixed[pl.ds(pl.multiple_of(step * block, block), block), :] = jnp.dot(
        matrix[...], scaled, preferred_element_type=jnp.float32
    )

    @pl.when(step == steps - 1)
    def finish():
        @pl.loop(0, block // 8)
        def butterfly(group):
            for tile in range(tiles):
                cols = slice(tile * LANES, (tile + 1) * LANES)
                spots = [
                    pl.ds(pl.multiple_of(index * block + group * 8, 8), 8)
                    for index in range(steps)
                ]
                values = [mixed[spot, cols] for spot in spots]
                gap = 1
                while gap < steps:
                    for index in range(steps):
                        if not index & gap:
                            above, below = values[index], values[index + gap]
                            values[index] = above + below
                            values[index + gap] = above - below
                    gap *= 2
                for spot, value in zip(spots, values):
                    mixed[spot, cols] = value

        @pl.loop(0, out_ref.shape[0] // 8)
        def gather(group):
            for lane in range(8):
                place = group * 8 + lane
                row = mixed[pl.ds(picks_ref[place], 1), :]
                out_ref[pl.ds(place, 1), :] = row * picks_sign_ref[place]


def front(design, weights, labels, signs, picks, picks_sign):
    rows_here, width = design.shape
    total = picks.shape[0]
    block = 256
    steps = rows_here // block
    lines = (steps, block // LANES, LANES)
    smem = pl.BlockSpec(memory_space=pltpu.SMEM)
    line = pl.BlockSpec((1,) + lines[1:], lambda i: (i, 0, 0))
    return pl.pallas_call(
        functools.partial(front_kernel, steps),
        grid=(steps,),
        out_shape=(
            jax.ShapeDtypeStruct(lines, jnp.float32),
            jax.ShapeDtypeStruct((8, width), jnp.float32),
            jax.ShapeDtypeStruct((total, width), jnp.float32),
        ),
        in_specs=[
            smem,
            smem,
            pl.BlockSpec((block, width), lambda i: (i, 0)),
            pl.BlockSpec((1, width), lambda i: (0, 0)),
            line,
            line,
        ],
        out_specs=(
            line,
            pl.BlockSpec((8, width), lambda i: (0, 0)),
            pl.BlockSpec((total, width), lambda i: (0, 0)),
        ),
        scratch_shapes=[
            pltpu.VMEM((block, block), jnp.bfloat16),
            pltpu.VMEM((rows_here, width), jnp.float32),
        ],
        name="front",
    )(picks, picks_sign, design, weights.reshape(1, width), labels.reshape(lines), signs.reshape(lines))


def tail_kernel(
    steps, count, design_ref, newton_ref, margins_ref, labels_ref, out_ref,
    held, slots, send_sem, recv_sem,
):
    step = pl.program_id(0)
    me = lax.axis_index("rows")
    block, width = design_ref.shape
    barrier = pltpu.get_barrier_semaphore()

    @pl.when(step == 0)
    def enter():
        held[...] = jnp.zeros_like(held)

        @pl.loop(1, count)
        def greet(turn):
            pl.semaphore_signal(
                barrier, inc=1, device_id=(lax.rem(me + turn, count),), device_id_type=MESH
            )

    newton = jnp.broadcast_to(newton_ref[...], (LANES, width)).astype(jnp.bfloat16)
    spread = lax.dot_general(
        design_ref[...], newton, (((1,), (1,)), ((), ())), preferred_element_type=jnp.float32
    )
    sub = lax.broadcasted_iota(jnp.int32, (8, LANES), 0)
    length = jnp.where(sub == 0, 1.0, jnp.where(sub == 1, 0.5, jnp.where(sub == 2, 0.25, 0.125)))
    loss = jnp.zeros((8, LANES), jnp.float32)
    for piece in range(block // LANES):
        along = spread[piece * LANES : (piece + 1) * LANES, :].T[:8, :]
        trial = margins_ref[0, piece : piece + 1, :] - length * along
        label = labels_ref[0, piece : piece + 1, :].astype(jnp.float32)
        soft = jnp.maximum(trial, 0.0) + jnp.log1p(jnp.exp(-jnp.abs(trial)))
        loss = loss + (soft - label * trial)
    held[...] += loss

    @pl.when(step == steps - 1)
    def combine():
        held[...] = jnp.broadcast_to(jnp.sum(held[...], axis=1, keepdims=True), (8, LANES))
        pl.semaphore_wait(barrier, count - 1)

        def copy(turn):
            return pltpu.make_async_remote_copy(
                src_ref=held,
                dst_ref=slots.at[me],
                send_sem=send_sem.at[turn],
                recv_sem=recv_sem.at[turn],
                device_id=(lax.rem(me + turn, count),),
                device_id_type=MESH,
            )

        @pl.loop(1, count)
        def send(turn):
            copy(turn).start()

        slots[me] = held[...]

        @pl.loop(1, count)
        def finish(turn):
            copy(turn).wait()

        out_ref[...] = jnp.sum(slots[...], axis=0)


def tail(design, newton_step, margins, labels, count):
    rows_here, width = design.shape
    block = 512
    steps = rows_here // block
    lines = (steps, block // LANES, LANES)
    line = pl.BlockSpec((1,) + lines[1:], lambda i: (i, 0, 0))
    return pl.pallas_call(
        functools.partial(tail_kernel, steps, count),
        grid=(steps,),
        out_shape=jax.ShapeDtypeStruct((8, LANES), jnp.float32),
        in_specs=[
            pl.BlockSpec((block, width), lambda i: (i, 0)),
            pl.BlockSpec((1, width), lambda i: (0, 0)),
            line,
            line,
        ],
        out_specs=pl.BlockSpec((8, LANES), lambda i: (0, 0)),
        scratch_shapes=[
            pltpu.VMEM((8, LANES), jnp.float32),
            pltpu.VMEM((count, 8, LANES), jnp.float32),
            pltpu.SemaphoreType.DMA((count,)),
            pltpu.SemaphoreType.DMA((count,)),
        ],
        compiler_params=pltpu.CompilerParams(collective_id=1, has_side_effects=True),
        name="tail",
    )(design, newton_step.reshape(1, width), margins.reshape(lines), labels.reshape(lines))


def exchange_kernel(
    orders, spans, part_ref, grad_ref, sketch_ref, gsum_ref,
    total, arrive_first, arrive_rest, grad_slots, grad_own,
    send_sem, recv_sem, back_send, back_recv, grad_send, grad_recv, own_sem,
):
    me = lax.axis_index("rows")
    steps = len(orders[0])
    rows = part_ref.shape[0]
    norm = 1.0 / math.sqrt(rows)
    half = rows // 2
    groups = range(len(orders))

    def peer(bit):
        return me ^ (1 << bit)

    def mine(bit):
        return (me >> bit) & 1

    core = orders[0][0]
    base = pl.multiple_of(mine(core) * half, half)
    other = pl.multiple_of((1 - mine(core)) * half, half)
    own_copies = []
    for group in groups:
        cols = slice(*spans[group])
        own_copies.append(
            pltpu.make_async_copy(
                part_ref.at[pl.ds(base, half), cols], total.at[:, cols], own_sem.at[group]
            )
        )
        own_copies[group].start()
    barrier = pltpu.get_barrier_semaphore()
    for bit in range(steps):
        pl.semaphore_signal(barrier, inc=1, device_id=(peer(bit),), device_id_type=MESH)
    pl.semaphore_wait(barrier, steps)

    def remote(source, target, out_sem, in_sem, bit):
        return pltpu.make_async_remote_copy(
            src_ref=source, dst_ref=target, send_sem=out_sem, recv_sem=in_sem,
            device_id=(peer(bit),), device_id_type=MESH,
        )

    sent = []
    pending = {}

    def start(copy, key):
        copy.start()
        sent.append(copy)
        pending[key] = copy

    def grad_start(step):
        source = grad_ref if step == 0 else grad_own.at[step - 1]
        start(
            remote(source, grad_slots.at[step], grad_send.at[step], grad_recv.at[step], step),
            ("grad", step),
        )

    def grad_finish(step):
        pending[("grad", step)].wait_recv()
        before = grad_ref[...] if step == 0 else grad_own[step - 1]
        grad_own[step] = before + grad_slots[step]

    grad_start(0)
    for group in groups:
        cols = slice(*spans[group])
        start(
            remote(
                part_ref.at[pl.ds(other, half), cols], arrive_first.at[:, cols],
                send_sem.at[0, group], recv_sem.at[0, group], core,
            ),
            (0, group),
        )

    offsets = [0 for group in groups]
    history = [[] for group in groups]

    def rest_start(step, group):
        cols = slice(*spans[group])
        size = half >> step
        bit = orders[group][step]
        place = half - (half >> (step - 1))
        history[group].append(offsets[group])
        away = pl.multiple_of(offsets[group] + (1 - mine(bit)) * size, size)
        start(
            remote(
                total.at[pl.ds(away, size), cols], arrive_rest.at[pl.ds(place, size), cols],
                send_sem.at[step, group], recv_sem.at[step, group], bit,
            ),
            (step, group),
        )
        offsets[group] = pl.multiple_of(offsets[group] + mine(bit) * size, size)

    for step in range(steps):
        if step > 0:
            grad_start(step)
        for group in groups:
            cols = slice(*spans[group])
            pending[(step, group)].wait_recv()
            if step == 0:
                own_copies[group].wait()
                total[:, cols] = total[:, cols] + arrive_first[:, cols]
            else:
                size = half >> step
                place = half - (half >> (step - 1))
                keep = pl.ds(offsets[group], size)
                total[keep, cols] = total[keep, cols] + arrive_rest[place : place + size, cols]
            if step + 1 < steps:
                rest_start(step + 1, group)
        grad_finish(step)

    def back_start(step, group):
        cols = slice(*spans[group])
        bit = orders[group][step]
        size = half >> step
        place = pl.ds(pl.multiple_of(base + offsets[group], size), size)
        start(
            remote(
                sketch_ref.at[place, cols], sketch_ref.at[place, cols],
                back_send.at[step, group], back_recv.at[step, group], bit,
            ),
            ("back", step, group),
        )

    last = half >> (steps - 1)
    for group in groups:
        cols = slice(*spans[group])
        place = pl.ds(pl.multiple_of(base + offsets[group], last), last)
        sketch_ref[place, cols] = (total[pl.ds(offsets[group], last), cols] * norm).astype(
            sketch_ref.dtype
        )
        back_start(steps - 1, group)
    for step in range(steps - 1, -1, -1):
        for group in groups:
            pending[("back", step, group)].wait_recv()
            if step > 0:
                offsets[group] = history[group][step - 1]
                back_start(step - 1, group)
    gsum_ref[...] = grad_own[steps - 1]
    for copy in sent:
        copy.wait_send()


def exchange(part, grad, count):
    rows, width = part.shape
    bits = count.bit_length() - 1
    rest = list(range(1, bits))
    tiles = width // LANES
    lanes = 3
    cuts = [-(-tiles * group // lanes) * LANES for group in range(lanes + 1)]
    spans = [(cuts[group], cuts[group + 1]) for group in range(lanes)]
    orders = []
    for group in range(lanes):
        turn = group * len(rest) // lanes
        orders.append([0] + rest[turn:] + rest[:turn])
    grid_sem = pltpu.SemaphoreType.DMA((bits, lanes))
    line_sem = pltpu.SemaphoreType.DMA((bits,))
    vmem = pl.BlockSpec(memory_space=pltpu.VMEM)
    return pl.pallas_call(
        functools.partial(exchange_kernel, orders, spans),
        out_shape=(
            jax.ShapeDtypeStruct((rows, width), jnp.bfloat16),
            jax.ShapeDtypeStruct(grad.shape, jnp.float32),
        ),
        in_specs=[pl.BlockSpec(memory_space=pl.ANY), vmem],
        out_specs=(vmem, vmem),
        scratch_shapes=[
            pltpu.VMEM((rows // 2, width), jnp.float32),
            pltpu.VMEM((rows // 2, width), jnp.float32),
            pltpu.VMEM((rows // 2, width), jnp.float32),
            pltpu.VMEM((bits,) + grad.shape, jnp.float32),
            pltpu.VMEM((bits,) + grad.shape, jnp.float32),
            grid_sem, grid_sem, grid_sem, grid_sem, line_sem, line_sem,
            pltpu.SemaphoreType.DMA((lanes,)),
        ],
        compiler_params=pltpu.CompilerParams(collective_id=2, has_side_effects=True),
        name="exchange",
    )(part, grad)


def solve_kernel(total_rows, piece_ref, gradient_ref, step_ref, hess, vec_r, vec_p, vec_q):
    width = piece_ref.shape[1]
    block = 256
    scale = 1.0 / total_rows
    for start in range(0, width, block):
        gram = lax.dot_general(
            piece_ref[:, start : start + block],
            piece_ref[...],
            (((0,), (0,)), ((), ())),
            preferred_element_type=jnp.float32,
        )
        row = lax.broadcasted_iota(jnp.int32, (block, width), 0) + start
        col = lax.broadcasted_iota(jnp.int32, (block, width), 1)
        hess[start : start + block, :] = gram * scale + jnp.where(row == col, ridge, 0.0)
    diag = jnp.zeros((1, width), jnp.float32)
    for start in range(0, width, block):
        row = lax.broadcasted_iota(jnp.int32, (block, width), 0) + start
        col = lax.broadcasted_iota(jnp.int32, (block, width), 1)
        diag = diag + jnp.sum(
            jnp.where(row == col, hess[start : start + block, :], 0.0), axis=0, keepdims=True
        )
    inverse = 1.0 / diag
    right = gradient_ref[...]
    vec_r[...] = right
    start_z = right * inverse
    vec_p[...] = start_z
    step_ref[...] = jnp.zeros_like(right)
    start_rz = jnp.sum(right * start_z, axis=1, keepdims=True)
    goal = jnp.max(start_rz) * 1e-13

    def product():
        tiles = width // LANES
        sums = [jnp.zeros((8, LANES), jnp.float32) for tile in range(tiles)]
        for piece in range(tiles):
            span = slice(piece * LANES, (piece + 1) * LANES)
            column = jnp.broadcast_to(vec_p[:, span], (LANES, LANES)).T
            for tile in range(tiles):
                prod = hess[span, tile * LANES : (tile + 1) * LANES] * column
                sums[tile] = sums[tile] + jnp.sum(prod.reshape(LANES // 8, 8, LANES), axis=0)
        for tile in range(tiles):
            vec_q[:, tile * LANES : (tile + 1) * LANES] = jnp.sum(
                sums[tile], axis=0, keepdims=True
            )

    def go(carry):
        done, level, rz = carry
        return jnp.logical_and(level > goal, done < 8 * width)

    def advance(carry):
        done, level, rz = carry
        product()
        direction, image = vec_p[...], vec_q[...]
        curve = jnp.sum(direction * image, axis=1, keepdims=True)
        alpha = jnp.where(curve > 0.0, rz / curve, 0.0)
        step_ref[...] = step_ref[...] + alpha * direction
        rest = vec_r[...] - alpha * image
        vec_r[...] = rest
        scaled_rest = rest * inverse
        next_rz = jnp.sum(rest * scaled_rest, axis=1, keepdims=True)
        beta = jnp.where(rz > 0.0, next_rz / rz, 0.0)
        vec_p[...] = scaled_rest + beta * direction
        return done + 1, jnp.max(next_rz), next_rz

    lax.while_loop(go, advance, (jnp.int32(0), jnp.max(start_rz), start_rz))


def newton_solve(piece, gradient, total_rows):
    width = piece.shape[1]
    vector = pltpu.VMEM((1, width), jnp.float32)
    return pl.pallas_call(
        functools.partial(solve_kernel, total_rows),
        out_shape=jax.ShapeDtypeStruct((1, width), jnp.float32),
        in_specs=[pl.BlockSpec(memory_space=pltpu.VMEM)] * 2,
        out_specs=pl.BlockSpec(memory_space=pltpu.VMEM),
        scratch_shapes=[pltpu.VMEM((width, width), jnp.float32), vector, vector, vector],
        name="newton_solve",
    )(piece, gradient.reshape(1, width)).reshape(width)


def body(design, weights, labels, signs, sample_rows):
    rows_here, width = design.shape
    device_count = lax.axis_size("rows")
    total_rows = rows_here * device_count
    owner_sign = parity_sign((sample_rows // rows_here) & lax.axis_index("rows"))
    margins, grad_part, own_part = front(
        design, weights, labels, signs, sample_rows % rows_here, owner_sign
    )
    piece, grad_sum = exchange(
        own_part, grad_part[0].reshape(width // LANES, LANES), device_count
    )
    gradient = grad_sum.reshape(width) / total_rows + ridge * weights
    newton_step = newton_solve(piece, gradient, total_rows)
    lengths = jnp.array([1.0, 0.5, 0.25, 0.125], jnp.float32)
    loss_total = tail(design, newton_step, margins, labels, device_count)[:4, 0]
    moved = weights[None, :] - lengths[:, None] * newton_step[None, :]
    losses = loss_total / total_rows + 0.5 * ridge * jnp.sum(moved * moved, axis=1)
    return (gradient, newton_step, losses)


def solution(mesh):
    placed = (P("rows", None), P(), P("rows"), P("rows"), P())
    return jax.shard_map(
        body, mesh=mesh, in_specs=placed, out_specs=(P(), P(), P()), check_vma=False
    )
```

```python
import functools
import math

import jax
import jax.numpy as jnp
from jax import lax
from jax.experimental import pallas as pl
from jax.experimental.pallas import tpu as pltpu
from jax.sharding import PartitionSpec as P

ridge = 0.05
LANES = 128
MESH = pl.DeviceIdType.MESH


def parity_sign(bits):
    for shift in (16, 8, 4, 2, 1):
        bits = bits ^ (bits >> shift)
    return (1 - 2 * (bits & 1)).astype(jnp.float32)


def front_kernel(
    steps, picks_ref, picks_sign_ref, design_ref, weights_ref, labels_ref, signs_ref,
    margins_ref, grad_out_ref, out_ref, matrix, mixed, grad_ref,
):
    step = pl.program_id(0)
    block, width = design_ref.shape
    tiles = width // LANES

    @pl.when(step == 0)
    def prepare():
        row = lax.broadcasted_iota(jnp.int32, (block, block), 0)
        col = lax.broadcasted_iota(jnp.int32, (block, block), 1)
        matrix[...] = parity_sign(row & col).astype(jnp.bfloat16)
        grad_ref[...] = jnp.zeros_like(grad_ref)

    weights = jnp.broadcast_to(weights_ref[...], (LANES, width)).astype(jnp.bfloat16)
    spread = lax.dot_general(
        design_ref[...], weights, (((1,), (1,)), ((), ())), preferred_element_type=jnp.float32
    )
    parts = []
    for piece in range(block // LANES):
        span = slice(piece * LANES, (piece + 1) * LANES)
        margin = spread[span, :].T[:8, :]
        margins_ref[0, piece : piece + 1, :] = margin[:1, :]
        prob = 1.0 / (1.0 + jnp.exp(-margin))
        label = labels_ref[0, piece : piece + 1, :].astype(jnp.float32)
        sign = signs_ref[0, piece : piece + 1, :].astype(jnp.float32)
        misfit = (prob - label).astype(jnp.bfloat16)
        grad_ref[...] += jnp.dot(
            misfit, design_ref[span, :], preferred_element_type=jnp.float32
        )
        factor = ((1.0 - 2.0 * sign) * jnp.sqrt(prob * (1.0 - prob)))[:1, :]
        column = jnp.broadcast_to(factor, (LANES, LANES)).T
        wide = jnp.concatenate([column] * tiles, axis=1)
        parts.append((design_ref[span, :].astype(jnp.float32) * wide).astype(jnp.bfloat16))
    scaled = jnp.concatenate(parts, axis=0)
    mixed[pl.ds(pl.multiple_of(step * block, block), block), :] = jnp.dot(
        matrix[...], scaled, preferred_element_type=jnp.float32
    )

    @pl.when(step == steps - 1)
    def finish():
        @pl.loop(0, block // 8)
        def butterfly(group):
            for tile in range(tiles):
                cols = slice(tile * LANES, (tile + 1) * LANES)
                spots = [
                    pl.ds(pl.multiple_of(index * block + group * 8, 8), 8)
                    for index in range(steps)
                ]
                values = [mixed[spot, cols] for spot in spots]
                gap = 1
                while gap < steps:
                    for index in range(steps):
                        if not index & gap:
                            above, below = values[index], values[index + gap]
                            values[index] = above + below
                            values[index + gap] = above - below
                    gap *= 2
                for spot, value in zip(spots, values):
                    mixed[spot, cols] = value

        grad_out_ref[...] = grad_ref[:1, :]

        @pl.loop(0, out_ref.shape[0] // 8)
        def gather(group):
            first = pl.multiple_of(group * 8, 8)
            cut = width // 2
            spots = [picks_ref[first + lane] for lane in range(8)]
            sub = lax.broadcasted_iota(jnp.int32, (8, cut), 0)
            sign = jnp.zeros((8, cut), jnp.float32)
            for lane in range(8):
                sign = jnp.where(sub == lane, picks_sign_ref[first + lane], sign)
            for start in (0, cut):
                cols = slice(start, start + cut)
                rows = jnp.zeros((8, cut), jnp.float32)
                for lane in range(8):
                    row = jnp.broadcast_to(mixed[pl.ds(spots[lane], 1), cols], (8, cut))
                    rows = jnp.where(sub == lane, row, rows)
                out_ref[pl.ds(first, 8), cols] = rows * sign


def front(design, weights, labels, signs, picks, picks_sign):
    rows_here, width = design.shape
    total = picks.shape[0]
    block = 256
    steps = rows_here // block
    lines = (steps, block // LANES, LANES)
    smem = pl.BlockSpec(memory_space=pltpu.SMEM)
    line = pl.BlockSpec((1,) + lines[1:], lambda i: (i, 0, 0))
    return pl.pallas_call(
        functools.partial(front_kernel, steps),
        grid=(steps,),
        out_shape=(
            jax.ShapeDtypeStruct(lines, jnp.float32),
            jax.ShapeDtypeStruct((1, width), jnp.float32),
            jax.ShapeDtypeStruct((total, width), jnp.float32),
        ),
        in_specs=[
            smem,
            smem,
            pl.BlockSpec((block, width), lambda i: (i, 0)),
            pl.BlockSpec((1, width), lambda i: (0, 0)),
            line,
            line,
        ],
        out_specs=(
            line,
            pl.BlockSpec((1, width), lambda i: (0, 0)),
            pl.BlockSpec((total, width), lambda i: (0, 0)),
        ),
        scratch_shapes=[
            pltpu.VMEM((block, block), jnp.bfloat16),
            pltpu.VMEM((rows_here, width), jnp.float32),
            pltpu.VMEM((8, width), jnp.float32),
        ],
        name="front",
    )(picks, picks_sign, design, weights.reshape(1, width), labels.reshape(lines), signs.reshape(lines))


def tail_kernel(
    steps, count, design_ref, newton_ref, margins_ref, labels_ref, out_ref,
    held, slots, send_sem, recv_sem,
):
    step = pl.program_id(0)
    me = lax.axis_index("rows")
    block, width = design_ref.shape
    barrier = pltpu.get_barrier_semaphore()

    @pl.when(step == 0)
    def enter():
        held[...] = jnp.zeros_like(held)

        @pl.loop(1, count)
        def greet(turn):
            pl.semaphore_signal(
                barrier, inc=1, device_id=(lax.rem(me + turn, count),), device_id_type=MESH
            )

    newton = jnp.broadcast_to(newton_ref[...], (LANES, width)).astype(jnp.bfloat16)
    spread = lax.dot_general(
        design_ref[...], newton, (((1,), (1,)), ((), ())), preferred_element_type=jnp.float32
    )
    sub = lax.broadcasted_iota(jnp.int32, (8, LANES), 0)
    length = jnp.where(sub == 0, 1.0, jnp.where(sub == 1, 0.5, jnp.where(sub == 2, 0.25, 0.125)))
    loss = jnp.zeros((8, LANES), jnp.float32)
    for piece in range(block // LANES):
        along = spread[piece * LANES : (piece + 1) * LANES, :].T[:8, :]
        trial = margins_ref[0, piece : piece + 1, :] - length * along
        label = labels_ref[0, piece : piece + 1, :].astype(jnp.float32)
        soft = jnp.maximum(trial, 0.0) + jnp.log1p(jnp.exp(-jnp.abs(trial)))
        loss = loss + (soft - label * trial)
    held[...] += loss

    @pl.when(step == steps - 1)
    def combine():
        held[...] = jnp.broadcast_to(jnp.sum(held[...], axis=1, keepdims=True), (8, LANES))
        pl.semaphore_wait(barrier, count - 1)

        def copy(turn):
            return pltpu.make_async_remote_copy(
                src_ref=held,
                dst_ref=slots.at[me],
                send_sem=send_sem.at[turn],
                recv_sem=recv_sem.at[turn],
                device_id=(lax.rem(me + turn, count),),
                device_id_type=MESH,
            )

        @pl.loop(1, count)
        def send(turn):
            copy(turn).start()

        slots[me] = held[...]

        @pl.loop(1, count)
        def finish(turn):
            copy(turn).wait()

        out_ref[...] = jnp.sum(slots[...], axis=0)


def tail(design, newton_step, margins, labels, count):
    rows_here, width = design.shape
    block = 512
    steps = rows_here // block
    lines = (steps, block // LANES, LANES)
    line = pl.BlockSpec((1,) + lines[1:], lambda i: (i, 0, 0))
    return pl.pallas_call(
        functools.partial(tail_kernel, steps, count),
        grid=(steps,),
        out_shape=jax.ShapeDtypeStruct((8, LANES), jnp.float32),
        in_specs=[
            pl.BlockSpec((block, width), lambda i: (i, 0)),
            pl.BlockSpec((1, width), lambda i: (0, 0)),
            line,
            line,
        ],
        out_specs=pl.BlockSpec((8, LANES), lambda i: (0, 0)),
        scratch_shapes=[
            pltpu.VMEM((8, LANES), jnp.float32),
            pltpu.VMEM((count, 8, LANES), jnp.float32),
            pltpu.SemaphoreType.DMA((count,)),
            pltpu.SemaphoreType.DMA((count,)),
        ],
        compiler_params=pltpu.CompilerParams(collective_id=1, has_side_effects=True),
        name="tail",
    )(design, newton_step.reshape(1, width), margins.reshape(lines), labels.reshape(lines))


def exchange_kernel(
    orders, spans, part_ref, grad_ref, sketch_ref, gsum_ref,
    total, arrive_first, arrive_rest, grad_slots, grad_own,
    send_sem, recv_sem, back_send, back_recv, grad_send, grad_recv, own_sem,
):
    me = lax.axis_index("rows")
    steps = len(orders[0])
    rows = part_ref.shape[0]
    norm = 1.0 / math.sqrt(rows)
    half = rows // 2
    groups = range(len(orders))

    def peer(bit):
        return me ^ (1 << bit)

    def mine(bit):
        return (me >> bit) & 1

    core = orders[0][0]
    base = pl.multiple_of(mine(core) * half, half)
    other = pl.multiple_of((1 - mine(core)) * half, half)
    own_copies = []
    for group in groups:
        cols = slice(*spans[group])
        own_copies.append(
            pltpu.make_async_copy(
                part_ref.at[pl.ds(base, half), cols], total.at[:, cols], own_sem.at[group]
            )
        )
        own_copies[group].start()
    barrier = pltpu.get_barrier_semaphore()
    for bit in range(steps):
        pl.semaphore_signal(barrier, inc=1, device_id=(peer(bit),), device_id_type=MESH)
    pl.semaphore_wait(barrier, steps)

    def remote(source, target, out_sem, in_sem, bit):
        return pltpu.make_async_remote_copy(
            src_ref=source, dst_ref=target, send_sem=out_sem, recv_sem=in_sem,
            device_id=(peer(bit),), device_id_type=MESH,
        )

    sent = []
    pending = {}

    def start(copy, key):
        copy.start()
        sent.append(copy)
        pending[key] = copy

    def grad_start(step):
        source = grad_ref if step == 0 else grad_own.at[step - 1]
        start(
            remote(source, grad_slots.at[step], grad_send.at[step], grad_recv.at[step], step),
            ("grad", step),
        )

    def grad_finish(step):
        pending[("grad", step)].wait_recv()
        before = grad_ref[...] if step == 0 else grad_own[step - 1]
        grad_own[step] = before + grad_slots[step]

    grad_start(0)
    for group in groups:
        cols = slice(*spans[group])
        start(
            remote(
                part_ref.at[pl.ds(other, half), cols], arrive_first.at[:, cols],
                send_sem.at[0, group], recv_sem.at[0, group], core,
            ),
            (0, group),
        )

    offsets = [0 for group in groups]
    history = [[] for group in groups]

    def rest_start(step, group):
        cols = slice(*spans[group])
        size = half >> step
        bit = orders[group][step]
        place = half - (half >> (step - 1))
        history[group].append(offsets[group])
        away = pl.multiple_of(offsets[group] + (1 - mine(bit)) * size, size)
        start(
            remote(
                total.at[pl.ds(away, size), cols], arrive_rest.at[pl.ds(place, size), cols],
                send_sem.at[step, group], recv_sem.at[step, group], bit,
            ),
            (step, group),
        )
        offsets[group] = pl.multiple_of(offsets[group] + mine(bit) * size, size)

    for step in range(steps):
        if step > 0:
            grad_start(step)
        for group in groups:
            cols = slice(*spans[group])
            pending[(step, group)].wait_recv()
            if step == 0:
                own_copies[group].wait()
                total[:, cols] = total[:, cols] + arrive_first[:, cols]
            else:
                size = half >> step
                place = half - (half >> (step - 1))
                keep = pl.ds(offsets[group], size)
                total[keep, cols] = total[keep, cols] + arrive_rest[place : place + size, cols]
            if step + 1 < steps:
                rest_start(step + 1, group)
        grad_finish(step)

    def back_start(step, group):
        cols = slice(*spans[group])
        bit = orders[group][step]
        size = half >> step
        place = pl.ds(pl.multiple_of(base + offsets[group], size), size)
        start(
            remote(
                sketch_ref.at[place, cols], sketch_ref.at[place, cols],
                back_send.at[step, group], back_recv.at[step, group], bit,
            ),
            ("back", step, group),
        )

    last = half >> (steps - 1)
    for group in groups:
        cols = slice(*spans[group])
        place = pl.ds(pl.multiple_of(base + offsets[group], last), last)
        sketch_ref[place, cols] = (total[pl.ds(offsets[group], last), cols] * norm).astype(
            sketch_ref.dtype
        )
        back_start(steps - 1, group)
    for step in range(steps - 1, -1, -1):
        for group in groups:
            pending[("back", step, group)].wait_recv()
            if step > 0:
                offsets[group] = history[group][step - 1]
                back_start(step - 1, group)
    gsum_ref[...] = grad_own[steps - 1]
    for copy in sent:
        copy.wait_send()


def exchange(part, grad, count):
    rows, width = part.shape
    bits = count.bit_length() - 1
    rest = list(range(1, bits))
    tiles = width // LANES
    lanes = tiles
    spans = [(group * LANES, (group + 1) * LANES) for group in range(lanes)]
    orders = []
    for group in range(lanes):
        turn = (group % 3) * len(rest) // 3
        orders.append([0] + rest[turn:] + rest[:turn])
    grid_sem = pltpu.SemaphoreType.DMA((bits, lanes))
    line_sem = pltpu.SemaphoreType.DMA((bits,))
    vmem = pl.BlockSpec(memory_space=pltpu.VMEM)
    return pl.pallas_call(
        functools.partial(exchange_kernel, orders, spans),
        out_shape=(
            jax.ShapeDtypeStruct((rows, width), jnp.bfloat16),
            jax.ShapeDtypeStruct(grad.shape, jnp.float32),
        ),
        in_specs=[pl.BlockSpec(memory_space=pl.ANY), vmem],
        out_specs=(vmem, vmem),
        scratch_shapes=[
            pltpu.VMEM((rows // 2, width), jnp.float32),
            pltpu.VMEM((rows // 2, width), jnp.float32),
            pltpu.VMEM((rows // 2, width), jnp.float32),
            pltpu.VMEM((bits,) + grad.shape, jnp.float32),
            pltpu.VMEM((bits,) + grad.shape, jnp.float32),
            grid_sem, grid_sem, grid_sem, grid_sem, line_sem, line_sem,
            pltpu.SemaphoreType.DMA((lanes,)),
        ],
        compiler_params=pltpu.CompilerParams(collective_id=2, has_side_effects=True),
        name="exchange",
    )(part, grad)


def solve_kernel(
    total_rows, piece_ref, gsum_ref, weights_ref, gradient_ref, step_ref,
    hess, vec_r, vec_p, vec_q,
):
    width = piece_ref.shape[1]
    block = 256
    scale = 1.0 / total_rows
    for start in range(0, width, block):
        gram = lax.dot_general(
            piece_ref[:, start : start + block],
            piece_ref[...],
            (((0,), (0,)), ((), ())),
            preferred_element_type=jnp.float32,
        )
        row = lax.broadcasted_iota(jnp.int32, (block, width), 0) + start
        col = lax.broadcasted_iota(jnp.int32, (block, width), 1)
        hess[start : start + block, :] = gram * scale + jnp.where(row == col, ridge, 0.0)
    diag = jnp.zeros((1, width), jnp.float32)
    for start in range(0, width, block):
        row = lax.broadcasted_iota(jnp.int32, (block, width), 0) + start
        col = lax.broadcasted_iota(jnp.int32, (block, width), 1)
        diag = diag + jnp.sum(
            jnp.where(row == col, hess[start : start + block, :], 0.0), axis=0, keepdims=True
        )
    inverse = 1.0 / diag
    right = gsum_ref[...] * scale + ridge * weights_ref[...]
    gradient_ref[...] = right
    vec_r[...] = right
    start_z = right * inverse
    vec_p[...] = start_z
    step_ref[...] = jnp.zeros_like(right)
    start_rz = jnp.sum(right * start_z, axis=1, keepdims=True)
    goal = jnp.max(start_rz) * 1e-13

    def product():
        tiles = width // LANES
        sums = [jnp.zeros((8, LANES), jnp.float32) for tile in range(tiles)]
        for piece in range(tiles):
            span = slice(piece * LANES, (piece + 1) * LANES)
            column = jnp.broadcast_to(vec_p[:, span], (LANES, LANES)).T
            for tile in range(tiles):
                prod = hess[span, tile * LANES : (tile + 1) * LANES] * column
                sums[tile] = sums[tile] + jnp.sum(prod.reshape(LANES // 8, 8, LANES), axis=0)
        for tile in range(tiles):
            vec_q[:, tile * LANES : (tile + 1) * LANES] = jnp.sum(
                sums[tile], axis=0, keepdims=True
            )

    def go(carry):
        done, level, rz = carry
        return jnp.logical_and(level > goal, done < 8 * width)

    def advance(carry):
        done, level, rz = carry
        product()
        direction, image = vec_p[...], vec_q[...]
        curve = jnp.sum(direction * image, axis=1, keepdims=True)
        alpha = jnp.where(curve > 0.0, rz / curve, 0.0)
        step_ref[...] = step_ref[...] + alpha * direction
        rest = vec_r[...] - alpha * image
        vec_r[...] = rest
        scaled_rest = rest * inverse
        next_rz = jnp.sum(rest * scaled_rest, axis=1, keepdims=True)
        beta = jnp.where(rz > 0.0, next_rz / rz, 0.0)
        vec_p[...] = scaled_rest + beta * direction
        return done + 1, jnp.max(next_rz), next_rz

    lax.while_loop(go, advance, (jnp.int32(0), jnp.max(start_rz), start_rz))


def newton_solve(piece, grad_sum, weights, total_rows):
    width = piece.shape[1]
    vector = pltpu.VMEM((1, width), jnp.float32)
    line = jax.ShapeDtypeStruct((1, width), jnp.float32)
    vmem = pl.BlockSpec(memory_space=pltpu.VMEM)
    gradient, step = pl.pallas_call(
        functools.partial(solve_kernel, total_rows),
        out_shape=(line, line),
        in_specs=[vmem] * 3,
        out_specs=(vmem, vmem),
        scratch_shapes=[pltpu.VMEM((width, width), jnp.float32), vector, vector, vector],
        name="newton_solve",
    )(piece, grad_sum, weights.reshape(1, width))
    return gradient.reshape(width), step.reshape(width)


def body(design, weights, labels, signs, sample_rows):
    rows_here, width = design.shape
    device_count = lax.axis_size("rows")
    total_rows = rows_here * device_count
    owner_sign = parity_sign((sample_rows // rows_here) & lax.axis_index("rows"))
    margins, grad_part, own_part = front(
        design, weights, labels, signs, sample_rows % rows_here, owner_sign
    )
    piece, grad_sum = exchange(own_part, grad_part, device_count)
    gradient, newton_step = newton_solve(piece, grad_sum, weights, total_rows)
    lengths = jnp.array([1.0, 0.5, 0.25, 0.125], jnp.float32)
    loss_total = tail(design, newton_step, margins, labels, device_count)[:4, 0]
    moved = weights[None, :] - lengths[:, None] * newton_step[None, :]
    losses = loss_total / total_rows + 0.5 * ridge * jnp.sum(moved * moved, axis=1)
    return (gradient, newton_step, losses)


def solution(mesh):
    placed = (P("rows", None), P(), P("rows"), P("rows"), P())
    return jax.shard_map(
        body, mesh=mesh, in_specs=placed, out_specs=(P(), P(), P()), check_vma=False
    )
```
